32 devices in a mesh: expert: 4 (over x, core), shard: 8 (over z, y).
Axes of the slice: x: 2, y: 2, z: 4, core: 2. Of those that a mesh axis runs over, the one named last changes fastest.
Arguments:
- train_down: float32 [16, 6400, 4096], P('expert', None, 'shard'), may hold values from -0.109375 to 0.109375
- other_down: bfloat16 [16, 6400, 4096], P('expert', None, 'shard'), may hold values from -0.0390625 to 0.0390625
- router_weight: float32 [4096, 16], P('shard', 'expert'), may hold values from -0.09375 to 0.09375
- router_gain: float32 [4096], P('shard'), may hold values from 0.25 to 1.75
Outputs:
- ready_down: bfloat16 [16, 6400, 4096], P('expert', 'shard')
- scale_down: float32 [16, 6400], P('expert', 'shard')
- serve_router: bfloat16 [4096, 16], replicated
The draws below stay inside these ranges and needn't reach their ends.
All inputs are finite; a program needn't handle non-finite values. Where the reference program divides by a largest or mean magnitude, that divisor is 1e-20 or more.
Results may differ from the reference program's by a relative error of at most 0.001.
Values may be sent and summed in bfloat16 or wider, within the bound.
No kernel may reach another device: no remote copies, remote signals or barrier semaphores. Data moves between devices by JAX's collectives and lax.ppermute only.
A program may use at most 256 MiB of HBM per device.

```python
import jax
import jax.numpy as jnp

EXPERTS = 16
D_MODEL = 4096
D_EXPERT = 6400


def spiked(array, rng, source, target, blocks, factor):
    owner, partner = [(jnp.arange(array.shape[axis_at]) // (array.shape[axis_at] // blocks)).reshape([-1 if axis == axis_at else 1 for axis in range(array.ndim)]) for axis_at in (source, target)]
    chosen = jax.random.permutation(rng, blocks)[partner]
    strong = (owner == chosen) | (owner == (partner + blocks // 2) % blocks)
    return jnp.where(strong, factor * array, array)


def block_levels(stream_key, dims, pieces, smallest, high):
    factor_of = 1.0
    for axis_at, parts in pieces:
        draws = jax.random.uniform(jax.random.fold_in(jax.random.fold_in(stream_key, 6), axis_at), (parts,), jnp.float32, smallest / len(pieces), high / len(pieces))
        factor_of = factor_of * jnp.repeat(jnp.exp(draws), dims[axis_at] // parts).reshape((-1,) + (1,) * (len(dims) - 1 - axis_at))
    return factor_of


def noise(key, dims, width, reach, pieces=(), dtype=jnp.bfloat16):
    drawn = width * jax.random.normal(key, dims, jnp.float32)
    if pieces:
        drawn = drawn * block_levels(key, dims, pieces, -0.22, 0.18)
    return jnp.clip(drawn, -reach, reach).astype(dtype)


def noise_with(rng, dims, width, reach, pieces, heavy, dtype=jnp.bfloat16):
    values = width * jax.random.normal(rng, dims, jnp.float32)
    if pieces:
        values = values * block_levels(rng, dims, pieces, -0.22, 0.18)
    return jnp.clip(spiked(values, jax.random.fold_in(rng, 3), *heavy), -reach, reach).astype(dtype)


def setup_inputs(seed: int = 0) -> dict:
    arg_keys = jax.random.split(jax.random.key(seed), 5)
    return {
        "train_down": noise_with(arg_keys[0], (EXPERTS, D_EXPERT, D_MODEL), D_EXPERT ** -0.5, 0.109375, ((0, 4), (2, 8)), (2, 1, 8, 2.0), jnp.float32),
        "other_down": noise(arg_keys[1], (EXPERTS, D_EXPERT, D_MODEL), (D_EXPERT * 4) ** -0.5, 0.0390625, ((0, 4), (2, 8))),
        "router_weight": noise(arg_keys[2], (D_MODEL, EXPERTS), D_MODEL ** -0.5, 0.09375, ((0, 8), (1, 4)), jnp.float32),
        "router_gain": jnp.clip(1.0 + 0.15 * jax.random.normal(arg_keys[3], (D_MODEL,), jnp.float32), 0.25, 1.75),
    }


def reference(train_down, other_down, router_weight, router_gain):
    latest_down = train_down + other_down.astype(jnp.float32)
    scale_down = jnp.max(jnp.abs(latest_down), axis=2)
    ready_down = (latest_down / jnp.expand_dims(scale_down, 2)).astype(jnp.bfloat16)
    serve_router = (router_weight * router_gain[:, None]).astype(jnp.bfloat16)
    return ready_down, scale_down, serve_router
```

```python
import functools

import jax
import jax.numpy as jnp
from jax import lax
from jax.experimental import pallas as pl
from jax.experimental.pallas import tpu as pltpu
from jax.sharding import PartitionSpec as P


def place_body(peers_ref, *refs, n, width, first):
    out_ref = refs[-1]
    for k in range(n):
        at = pl.multiple_of(peers_ref[k] * width, 128)
        out_ref[0, :, pl.ds(at, width)] = refs[k][...]


def place(peers, pieces, ready, e, shape):
    n, (rows, width) = len(pieces), pieces[0].shape
    steps = 5
    block = rows // steps
    first = ready is None
    in_specs = [pl.BlockSpec((block, width), lambda i, p: (i, 0)) for _ in pieces]
    operands = [peers, *pieces]
    aliases = {}
    if not first:
        in_specs.append(pl.BlockSpec(memory_space=pl.ANY))
        operands.append(ready)
        aliases = {n + 1: 0}
    return pl.pallas_call(
        functools.partial(place_body, n=n, width=width, first=first),
        grid_spec=pltpu.PrefetchScalarGridSpec(
            num_scalar_prefetch=1,
            grid=(steps,),
            in_specs=in_specs,
            out_specs=pl.BlockSpec((1, block, n * width), lambda i, p: (e, i, 0)),
        ),
        out_shape=jax.ShapeDtypeStruct(shape, jnp.bfloat16),
        input_output_aliases=aliases,
    )(*operands)


def doubled(x, axis_name, n, axis, after=None):
    me = lax.axis_index(axis_name)
    bit = 1
    while bit < n:
        other = lax.ppermute(x, axis_name, [(i, i ^ bit) for i in range(n)])
        if after is not None and bit == 1:
            x, other, after = lax.optimization_barrier((x, other, after))
        upper = (me & bit) != 0
        x = jnp.concatenate([jnp.where(upper, other, x), jnp.where(upper, x, other)], axis=axis)
        bit *= 2
    return x, after


def per_device(train_down, other_down, router_weight, router_gain, n, m):
    experts, all_rows, width = train_down.shape
    rows = all_rows // n
    me = lax.axis_index("shard")
    peers = jnp.stack([me ^ k for k in range(n)]).astype(jnp.int32)

    part_router = (router_weight * router_gain[:, None]).astype(jnp.bfloat16).T
    latest_down = train_down + other_down.astype(jnp.float32)
    tops = jnp.max(jnp.abs(latest_down), axis=2)
    serve_router, tops = doubled(part_router, "shard", n, 1, tops)
    serve_router = doubled(serve_router, "expert", m, 0)[0].T
    bit = 1
    while bit < n:
        tops = jnp.maximum(tops, lax.ppermute(tops, "shard", [(i, i ^ bit) for i in range(n)]))
        bit *= 2
    scale_down = lax.dynamic_slice_in_dim(tops, me * rows, rows, axis=1)
    tops, serve_router = lax.optimization_barrier((tops, serve_router))

    halves = (list(range(n // 2, n)), list(range(n // 2)))
    ready = None
    waiting = []
    for e in range(experts):
        if e >= 2:
            ready = place(peers, waiting[e - 2], ready, e - 2, (experts, rows, n * width))
            ready, tops = lax.optimization_barrier((ready, tops))
        pieces = [None] * n
        for half in halves:
            local = {}
            for k in half:
                at = (me ^ k) * rows
                new = lax.dynamic_slice(train_down, (e, at, 0), (1, rows, width))[0]
                new = new + lax.dynamic_slice(other_down, (e, at, 0), (1, rows, width))[0].astype(jnp.float32)
                own = lax.dynamic_slice(tops, (e, at), (1, rows))[0]
                local[k] = (new / own[:, None]).astype(jnp.bfloat16)
            *out, tops = lax.optimization_barrier((*local.values(), tops))
            for k, piece in zip(half, out):
                pieces[k] = lax.ppermute(piece, "shard", [(i, i ^ k) for i in range(n)]) if k else piece
        waiting.append(pieces)
    for e in range(max(experts - 2, 0), experts):
        ready = place(peers, waiting[e], ready, e, (experts, rows, n * width))
    return (ready, scale_down, serve_router)


def solution(mesh):
    in_specs = (
        P("expert", None, "shard"),
        P("expert", None, "shard"),
        P("shard", "expert"),
        P("shard"),
    )
    out_specs = (P("expert", "shard", None), P("expert", "shard"), P())
    return jax.shard_map(
        functools.partial(per_device, n=mesh.shape["shard"], m=mesh.shape["expert"]),
        mesh=mesh, in_specs=in_specs, out_specs=out_specs, check_vma=False,
    )
```
